32 devices in a mesh: seq: 8 (over y, x, core), head: 4 (over z).
Axes of the slice: x: 2, y: 2, z: 4, core: 2. Of those that a mesh axis runs over, the one named last changes fastest.
Arguments:
- tokens: bfloat16 [32, 1024, 1024], P('seq'), may hold values from -6 to 6
- w_query: bfloat16 [1024, 1024], P(None, 'head'), may hold values from -1 to 1
- w_key: bfloat16 [1024, 1024], P(None, 'head'), may hold values from -1 to 1
- w_value: bfloat16 [1024, 1024], P(None, 'head'), may hold values from -0.1875 to 0.1875
- w_out: bfloat16 [1024, 1024], P('head'), may hold values from -0.1875 to 0.1875
Outputs:
- mixed: bfloat16 [32, 1024, 1024], P('seq', None, 'head')
The draws below stay inside these ranges and needn't reach their ends.
All inputs are finite; a program needn't handle non-finite values.
Results may differ from the reference program's by a relative error of at most 0.012.
Values may be sent and summed in bfloat16 or wider, within the bound.
A program may use at most 128 MiB of HBM per device.

```python
import jax
import jax.numpy as jnp
from jax import lax

D = 1024
HEADS = 16
FRAMES = 32
PATCHES = 1024


def query_key_pair(key):
    shape_full = (D, D)
    base = jnp.clip(jax.random.normal(jax.random.fold_in(key, 11), shape_full, jnp.float32), -6.0, 6.0)
    other = jnp.clip(jax.random.normal(jax.random.fold_in(key, 12), shape_full, jnp.float32), -6.0, 6.0)
    return (base * D ** (-0.5), other * D ** (-0.5))


def draw_w_query(key, part):
    first, second = query_key_pair(key)
    return first.astype(jnp.bfloat16)


def draw_w_key(key, part):
    first, second = query_key_pair(key)
    return second.astype(jnp.bfloat16)


def steps_of(own_key, extent, shards, low, high):
    level = 1.0
    for dim, parts in shards:
        draws = jax.random.uniform(jax.random.fold_in(jax.random.fold_in(own_key, 6), dim), (parts,), jnp.float32, low / len(shards), high / len(shards))
        level = level * jnp.repeat(jnp.exp(draws), extent[dim] // parts).reshape((-1,) + (1,) * (len(extent) - 1 - dim))
    return level


def noise(rng, extent, spread, limit, split=(), dtype=jnp.bfloat16):
    array = spread * jax.random.normal(rng, extent, jnp.float32)
    if split:
        array = array * steps_of(rng, extent, split, -0.22, 0.18)
    return jnp.clip(array, -limit, limit).astype(dtype)


def setup_inputs(seed: int = 0) -> dict:
    streams_of = jax.random.split(jax.random.key(seed), 6)
    tokens = noise(streams_of[0], (FRAMES, PATCHES, D), 1.0, 6.0, ((0, 8),))
    w_query = draw_w_query(jax.random.fold_in(streams_of[5], 71), 0)
    w_key = draw_w_key(jax.random.fold_in(streams_of[5], 71), 0)
    w_value = noise(streams_of[3], (D, D), D ** -0.5, 0.1875, ((1, 4),))
    w_out = noise(streams_of[4], (D, D), D ** -0.5, 0.1875, ((0, 4),))
    return {"tokens": tokens, "w_query": w_query, "w_key": w_key, "w_value": w_value, "w_out": w_out}


epsilon = 1e-05

def normalize(tokens):
    values = tokens.astype(jnp.float32)
    row_mean = lax.optimization_barrier(jnp.mean(values, axis=-1, keepdims=True))
    centered = values - row_mean
    row_var = lax.optimization_barrier(jnp.mean(centered * centered, axis=-1, keepdims=True))
    return (centered * lax.rsqrt(row_var + epsilon)).astype(jnp.bfloat16)

def project(source, weight):
    frames, patch_count, width = source.shape
    flat = jnp.dot(source.reshape(frames * patch_count, width), weight, preferred_element_type=jnp.float32)
    return flat.astype(jnp.bfloat16).reshape(frames, patch_count, weight.shape[1])

def attend(queries, key_rows, value_rows, head_count):
    frames, patch_count, feature_width = queries.shape
    head_size = feature_width // head_count
    query_flat = queries.reshape(frames, patch_count * head_count, head_size).astype(jnp.float32)
    key_flat = key_rows.reshape(frames, patch_count * head_count, head_size).astype(jnp.float32)
    value_flat = value_rows.reshape(frames, patch_count * head_count, head_size).astype(jnp.float32)
    scores = jnp.einsum('fmd,gmd->fgm', query_flat, key_flat) * head_size ** (-0.5)
    row_top = lax.optimization_barrier(jnp.max(scores, axis=1, keepdims=True))
    raised = jnp.exp(scores - row_top)
    weights = (raised / lax.optimization_barrier(jnp.sum(raised, axis=1, keepdims=True))).astype(jnp.bfloat16)
    attended = jnp.einsum('fgm,gmd->fmd', weights.astype(jnp.float32), value_flat)
    return attended.astype(jnp.bfloat16).reshape(frames, patch_count, feature_width)

def reference(tokens, w_query, w_key, w_value, w_out):
    normed = normalize(tokens)
    queries = project(normed, w_query)
    key_rows = project(normed, w_key)
    value_rows = project(normed, w_value)
    attended = attend(queries, key_rows, value_rows, HEADS)
    return project(attended, w_out)
```

```python
import jax
import jax.numpy as jnp
from jax import lax
from jax.sharding import PartitionSpec as P

HS = 64


epsilon = 1e-05


def normalize(tokens):
    values = tokens.astype(jnp.float32)
    row_mean = jnp.mean(values, axis=-1, keepdims=True)
    centered = values - row_mean
    row_var = jnp.mean(centered * centered, axis=-1, keepdims=True)
    return (centered * lax.rsqrt(row_var + epsilon)).astype(jnp.bfloat16)


def attend(queries, key_rows, value_rows, head_count):
    frames, patch_count, feature_width = queries.shape
    head_size = feature_width // head_count
    query_flat = queries.reshape(frames, patch_count * head_count, head_size)
    key_flat = key_rows.reshape(frames, patch_count * head_count, head_size)
    value_flat = value_rows.reshape(frames, patch_count * head_count, head_size)
    scores = jnp.einsum(
        "fmd,gmd->fgm", query_flat, key_flat, preferred_element_type=jnp.float32
    ) * head_size ** (-0.5)
    row_top = jnp.max(scores, axis=1, keepdims=True)
    raised = jnp.exp(scores - row_top)
    weights = (raised / jnp.sum(raised, axis=1, keepdims=True)).astype(jnp.bfloat16)
    attended = jnp.einsum("fgm,gmd->fmd", weights, value_flat, preferred_element_type=jnp.float32)
    return attended.astype(jnp.bfloat16).reshape(frames, patch_count, feature_width)


def local(tokens, w_query, w_key, w_value, w_out):
    seq, head = lax.axis_size("seq"), lax.axis_size("head")
    row, column = lax.axis_index("seq"), lax.axis_index("head")
    quarter = tokens.shape[1] // head
    own = lax.dynamic_slice_in_dim(tokens, column * quarter, quarter, axis=1)
    width, group = w_query.shape
    stacked = jnp.stack(
        [
            lax.dynamic_slice_in_dim(w, row * (width // seq), width // seq, axis=0)
            for w in (w_query, w_key, w_value)
        ]
    )
    weights = lax.all_gather(stacked, ("head", "seq"))
    weights = weights.reshape(head, seq, 3, width // seq, group)
    share = w_out.shape[0] // seq
    out_part = lax.dynamic_slice_in_dim(w_out, row * share, share, axis=0)
    out_all = lax.all_gather(out_part, ("head", "seq"), axis=0, tiled=True)
    mine = lax.all_to_all(own, "seq", split_axis=1, concat_axis=0, tiled=True)
    frames, patches, _ = mine.shape
    normed = normalize(mine)

    def project(index):
        w = weights[:, :, index].transpose(1, 2, 0, 3).reshape(width, head * group)
        flat = jnp.dot(
            normed.reshape(frames * patches, width), w, preferred_element_type=jnp.float32
        )
        return flat.astype(jnp.bfloat16).reshape(frames, patches, head * group)

    attended = attend(project(0), project(1), project(2), head * group // HS)
    mixed = jnp.dot(
        attended.reshape(frames * patches, head * group), out_all, preferred_element_type=jnp.float32
    )
    mixed = mixed.astype(jnp.bfloat16).reshape(frames, patches, width)
    mixed = lax.all_to_all(mixed, "seq", split_axis=0, concat_axis=1, tiled=True)
    return lax.all_to_all(mixed, "head", split_axis=2, concat_axis=1, tiled=True)


def solution(mesh):
    return jax.shard_map(
        local,
        mesh=mesh,
        in_specs=(
            P("seq", None, None),
            P(None, "head"),
            P(None, "head"),
            P(None, "head"),
            P("head", None),
        ),
        out_specs=P("seq", None, "head"),
        check_vma=False,
    )
```

```python
import functools

import jax
import jax.numpy as jnp
from jax import lax
from jax.experimental import pallas as pl
from jax.experimental.pallas import tpu as pltpu
from jax.sharding import PartitionSpec as P

HS = 64
EPSILON = 1e-05
SUB = 8
MASKED = -1e30
MESH = pl.DeviceIdType.MESH


def drain(ref, sem):
    pltpu.make_async_copy(ref, ref, sem).wait()


def kernel(
    seq, head,
    tok, wq, wk, wv, wo, out,
    x, normed, qkv, w, w_o, att, mixed, bias,
    tok_send, tok_recv, load_sem, s1_send, s1_recv, s2_send, s2_recv, s3_send, s3_recv,
    o1_send, o1_recv, o2_send, o2_recv, out_send, out_recv,
):
    s, z = lax.axis_index("seq"), lax.axis_index("head")
    groups, frames = x.shape[0], x.shape[1]
    own_frames = tok.shape[0]
    width = tok.shape[2]
    columns = wq.shape[1]
    rows = frames * SUB
    own_patches = groups * SUB
    quarter = seq * own_patches
    slice_rows = width // seq
    half_seq = seq // 2
    parity, place = lax.rem(s, 2), s // 2
    sibling = s + 1 - 2 * parity
    total = seq * head

    def send(src, dst, send_sem, recv_sem, to_s, to_z):
        pltpu.make_async_remote_copy(
            src_ref=src, dst_ref=dst, send_sem=send_sem, recv_sem=recv_sem,
            device_id=(to_s, to_z), device_id_type=MESH,
        ).start()

    def tok_block(to_s, g):
        start = pl.multiple_of(z * quarter + to_s * own_patches + g * SUB, SUB)
        return tok.at[:, pl.ds(start, SUB), :]

    slice_start = pl.multiple_of((parity * half_seq + place) * slice_rows, slice_rows)
    my_slice = pl.ds(slice_start, slice_rows)
    weights = (wq, wk, wv)
    for j in range(3):
        for i in range(1, head):
            send(
                weights[j].at[my_slice, :], w.at[j, z, my_slice, :],
                s1_send.at[j], s1_recv.at[j, i - 1], s, lax.rem(z + i, head),
            )
    for i in range(1, seq):
        to_s = lax.rem(s + i, seq)
        for g in range(groups):
            send(
                tok_block(to_s, g), x.at[g, pl.ds(s * own_frames, own_frames)],
                tok_send.at[g], tok_recv.at[g], to_s, z,
            )
    for g in range(groups):
        pltpu.make_async_copy(
            tok_block(s, g), x.at[g, pl.ds(s * own_frames, own_frames)], tok_recv.at[g]
        ).start()
    shard = width // head
    half = shard // 2
    for i in range(1, head):
        send(
            wo.at[pl.ds(pl.multiple_of(parity * half, half), half), :],
            w_o.at[pl.ds(pl.multiple_of(z * shard + parity * half, half), half), :],
            o1_send, o1_recv.at[i - 1], s, lax.rem(z + i, head),
        )
    own = [pltpu.make_async_copy(weights[j], w.at[j, z], load_sem.at[j]) for j in range(3)]
    own.append(
        pltpu.make_async_copy(
            wo, w_o.at[pl.ds(pl.multiple_of(z * shard, shard), shard), :], load_sem.at[3]
        )
    )
    for copy in own:
        copy.start()

    row = lax.broadcasted_iota(jnp.int32, (rows, rows), 0)
    col = lax.broadcasted_iota(jnp.int32, (rows, rows), 1)
    bias[...] = jnp.where((row & (SUB - 1)) == (col & (SUB - 1)), 0.0, MASKED)

    for j in range(3):
        for i in range(1, head):
            from_z = lax.rem(z + head - i, head)
            piece = w.at[j, from_z, my_slice, :]
            drain(piece, s1_recv.at[j, i - 1])
            for k in range(1, half_seq):
                to_s = lax.rem(place + k, half_seq) * 2 + parity
                send(piece, piece, s2_send.at[j], s2_recv.at[j], to_s, z)

    step_frames = 8
    for g in range(groups):
        drain(x.at[g], tok_recv.at[g])

        @pl.loop(0, frames // step_frames)
        def _(c):
            block = x[g, pl.ds(c * step_frames, step_frames)].astype(jnp.float32)
            values = block.reshape(step_frames * SUB, width)
            mean = jnp.mean(values, axis=-1, keepdims=True)
            centered = values - mean
            var = jnp.mean(centered * centered, axis=-1, keepdims=True)
            start = pl.multiple_of(c * step_frames * SUB, step_frames * SUB)
            normed[g, pl.ds(start, step_frames * SUB), :] = (
                centered * lax.rsqrt(var + EPSILON)
            ).astype(jnp.bfloat16)

    def project(j, g):
        @pl.loop(0, head)
        def _(h):
            r = jnp.dot(normed[g], w[j, h], preferred_element_type=jnp.float32)
            if j == 0:
                r = r * HS ** (-0.5)
            start = pl.multiple_of(h * columns, columns)
            qkv[j, g, :, pl.ds(start, columns)] = r.astype(jnp.bfloat16)

    parity_rows = pl.ds(
        pl.multiple_of(parity * half_seq * slice_rows, slice_rows), half_seq * slice_rows
    )
    for j in range(3):
        own[j].wait()
        drain(
            w.at[j, pl.ds(0, head - 1), pl.ds(0, (half_seq - 1) * slice_rows), :], s2_recv.at[j]
        )
        for i in range(1, head):
            piece = w.at[j, lax.rem(z + i, head), parity_rows, :]
            send(piece, piece, s3_send.at[j], s3_recv.at[j], sibling, z)
        if j == 1:
            for i in range(1, head):
                from_z = lax.rem(z + head - i, head)
                piece = w_o.at[
                    pl.ds(pl.multiple_of(from_z * shard + parity * half, half), half), :
                ]
                drain(piece, o1_recv.at[i - 1])
                send(piece, piece, o2_send, o2_recv, sibling, z)
        drain(w.at[j, pl.ds(0, head - 1), pl.ds(0, half_seq * slice_rows), :], s3_recv.at[j])
        if j < 2:

            @pl.loop(0, groups)
            def _(g):
                project(j, g)

    own[3].wait()
    drain(w_o.at[pl.ds(0, (head - 1) * half), :], o2_recv)

    pair = 2 * HS
    left = lax.broadcasted_iota(jnp.int32, (rows, pair), 1) < HS
    left_b = left.astype(jnp.float32).astype(jnp.bfloat16)
    right_b = (1.0 - left.astype(jnp.float32)).astype(jnp.bfloat16)
    ones = jnp.ones((rows, pair), jnp.bfloat16)
    me = s * head + z

    def out_block(g):
        start = pl.multiple_of(z * quarter + s * own_patches + g * SUB, SUB)
        return out.at[:, pl.ds(start, SUB), :]

    @pl.loop(0, groups)
    def _(g):
        project(2, g)

        @pl.loop(0, width // pair)
        def _(n):
            lanes = pl.ds(pl.multiple_of(n * pair, pair), pair)
            q, k, v = qkv[0, g, :, lanes], qkv[1, g, :, lanes], qkv[2, g, :, lanes]
            v_ones = jnp.concatenate([v, ones], axis=1)
            results = []
            for mask in (left_b, right_b):
                score = lax.dot_general(
                    q * mask, k, (((1,), (1,)), ((), ())), preferred_element_type=jnp.float32
                )
                score = score + bias[...]
                top = jnp.max(score, axis=1, keepdims=True)
                raised = jnp.exp(score - top).astype(jnp.bfloat16)
                r = jnp.dot(raised, v_ones, preferred_element_type=jnp.float32)
                results.append(r[:, :pair] / r[:, pair:])
            att[:, lanes] = jnp.where(left, results[0], results[1]).astype(jnp.bfloat16)

        @pl.loop(0, head)
        def _(h):
            lanes = pl.ds(pl.multiple_of(h * columns, columns), columns)
            r = jnp.dot(att[...], w_o[:, lanes], preferred_element_type=jnp.float32)
            mixed[g, pl.ds(h * frames, frames)] = r.reshape(frames, SUB, columns).astype(
                jnp.bfloat16
            )

        @pl.loop(1, total)
        def _(i):
            to = lax.rem(me + i, total)
            to_s, to_z = to // head, lax.rem(to, head)
            send(
                mixed.at[g, pl.ds(to_z * frames + to_s * own_frames, own_frames)],
                out_block(g), out_send.at[g], out_recv, to_s, to_z,
            )

        pltpu.make_async_copy(
            mixed.at[g, pl.ds(z * frames + s * own_frames, own_frames)], out_block(g), out_recv
        ).start()

    drain(out, out_recv)
    blocks = head * frames
    for g in range(groups):
        drain(mixed.at[g, pl.ds(0, blocks - blocks // total)], out_send.at[g])
        drain(x.at[g, pl.ds(0, frames - own_frames)], tok_send.at[g])
    for j in range(3):
        drain(w.at[j, pl.ds(0, head - 1), pl.ds(0, slice_rows), :], s1_send.at[j])
        drain(
            w.at[j, pl.ds(0, head - 1), pl.ds(0, (half_seq - 1) * slice_rows), :], s2_send.at[j]
        )
        drain(w.at[j, pl.ds(0, head - 1), pl.ds(0, half_seq * slice_rows), :], s3_send.at[j])
    drain(w_o.at[pl.ds(0, (head - 1) * half), :], o1_send)
    drain(w_o.at[pl.ds(0, (head - 1) * half), :], o2_send)


def local(tokens, w_query, w_key, w_value, w_out):
    seq, head = lax.axis_size("seq"), lax.axis_size("head")
    own_frames, patches, width = tokens.shape
    frames = own_frames * seq
    groups = patches // (seq * head * SUB)
    rows = frames * SUB
    columns = w_query.shape[1]
    bf16 = jnp.bfloat16
    dma = pltpu.SemaphoreType.DMA
    return pl.pallas_call(
        functools.partial(kernel, seq, head),
        out_shape=jax.ShapeDtypeStruct((own_frames, patches, width // head), bf16),
        in_specs=[pl.BlockSpec(memory_space=pl.ANY)] * 5,
        out_specs=pl.BlockSpec(memory_space=pl.ANY),
        scratch_shapes=[
            pltpu.VMEM((groups, frames, SUB, width), bf16),
            pltpu.VMEM((groups, rows, width), bf16),
            pltpu.VMEM((3, groups, rows, width), bf16),
            pltpu.VMEM((3, head, width, columns), bf16),
            pltpu.VMEM((width, width), bf16),
            pltpu.VMEM((rows, width), bf16),
            pltpu.VMEM((groups, head * frames, SUB, width // head), bf16),
            pltpu.VMEM((rows, rows), jnp.float32),
            dma((groups,)), dma((groups,)), dma((4,)),
            dma((3,)), dma((3, head - 1)), dma((3,)), dma((3,)), dma((3,)), dma((3,)),
            dma, dma((head - 1,)), dma, dma, dma((groups,)), dma,
        ],
        compiler_params=pltpu.CompilerParams(
            has_side_effects=True, vmem_limit_bytes=60 * 1024 * 1024
        ),
    )(tokens, w_query, w_key, w_value, w_out)


def solution(mesh):
    return jax.shard_map(
        local,
        mesh=mesh,
        in_specs=(
            P("seq", None, None),
            P(None, "head"),
            P(None, "head"),
            P(None, "head"),
            P("head", None),
        ),
        out_specs=P("seq", None, "head"),
        check_vma=False,
    )
```

```python
import functools

import jax
import jax.numpy as jnp
from jax import lax
from jax.experimental import pallas as pl
from jax.experimental.pallas import tpu as pltpu
from jax.sharding import PartitionSpec as P

HS = 64
EPSILON = 1e-05
SUB = 8
MASKED = -1e30
MESH = pl.DeviceIdType.MESH


def drain(ref, sem):
    pltpu.make_async_copy(ref, ref, sem).wait()


def kernel(
    seq, head,
    tok, wq, wk, wv, wo, out,
    x, normed, qkv, w, w_o, att, mixed, bias,
    tok_send, tok_recv, load_sem, s1_send, s1_recv, s2_send, s2_recv, s3_send, s3_recv,
    o1_send, o1_recv, o2_send, o2_recv, out_send, out_recv,
):
    s, z = lax.axis_index("seq"), lax.axis_index("head")
    groups, frames = x.shape[0], x.shape[1]
    own_frames = tok.shape[0]
    width = tok.shape[2]
    columns = wq.shape[1]
    rows = frames * SUB
    own_patches = groups * SUB
    quarter = seq * own_patches
    slice_rows = width // seq
    half_seq = seq // 2
    parity, place = lax.rem(s, 2), s // 2
    sibling = s + 1 - 2 * parity
    total = seq * head

    def send(src, dst, send_sem, recv_sem, to_s, to_z):
        pltpu.make_async_remote_copy(
            src_ref=src, dst_ref=dst, send_sem=send_sem, recv_sem=recv_sem,
            device_id=(to_s, to_z), device_id_type=MESH,
        ).start()

    def tok_block(to_s, g):
        start = pl.multiple_of(z * quarter + to_s * own_patches + g * SUB, SUB)
        return tok.at[:, pl.ds(start, SUB), :]

    slice_start = pl.multiple_of((parity * half_seq + place) * slice_rows, slice_rows)
    my_slice = pl.ds(slice_start, slice_rows)
    weights = (wq, wk, wv)
    for j in range(3):
        for i in range(1, head):
            send(
                weights[j].at[my_slice, :], w.at[j, z, my_slice, :],
                s1_send.at[j], s1_recv.at[j, i - 1], s, lax.rem(z + i, head),
            )
    def exchange(g):
        for i in range(1, seq):
            to_s = lax.rem(s + i, seq)
            send(
                tok_block(to_s, g), x.at[g, pl.ds(s * own_frames, own_frames)],
                tok_send.at[g], tok_recv.at[g], to_s, z,
            )
        pltpu.make_async_copy(
            tok_block(s, g), x.at[g, pl.ds(s * own_frames, own_frames)], tok_recv.at[g]
        ).start()

    exchange(0)
    shard = width // head
    half = shard // 2
    for i in range(1, head):
        send(
            wo.at[pl.ds(pl.multiple_of(parity * half, half), half), :],
            w_o.at[pl.ds(pl.multiple_of(z * shard + parity * half, half), half), :],
            o1_send, o1_recv.at[i - 1], s, lax.rem(z + i, head),
        )
    own = [pltpu.make_async_copy(weights[j], w.at[j, z], load_sem.at[j]) for j in range(3)]
    own.append(
        pltpu.make_async_copy(
            wo, w_o.at[pl.ds(pl.multiple_of(z * shard, shard), shard), :], load_sem.at[3]
        )
    )
    for copy in own:
        copy.start()

    row = lax.broadcasted_iota(jnp.int32, (rows, rows), 0)
    col = lax.broadcasted_iota(jnp.int32, (rows, rows), 1)
    bias[...] = jnp.where((row & (SUB - 1)) == (col & (SUB - 1)), 0.0, MASKED)

    for j in range(3):
        for i in range(1, head):
            from_z = lax.rem(z + head - i, head)
            piece = w.at[j, from_z, my_slice, :]
            drain(piece, s1_recv.at[j, i - 1])
            for k in range(1, half_seq):
                to_s = lax.rem(place + k, half_seq) * 2 + parity
                send(piece, piece, s2_send.at[j], s2_recv.at[j], to_s, z)

    for g in range(1, groups):
        exchange(g)

    step_frames = 8

    def norm(g):
        drain(x.at[g], tok_recv.at[g])

        @pl.loop(0, frames // step_frames)
        def _(c):
            block = x[g, pl.ds(c * step_frames, step_frames)].astype(jnp.float32)
            values = block.reshape(step_frames * SUB, width)
            mean = jnp.mean(values, axis=-1, keepdims=True)
            centered = values - mean
            var = jnp.mean(centered * centered, axis=-1, keepdims=True)
            start = pl.multiple_of(c * step_frames * SUB, step_frames * SUB)
            normed[pl.ds(start, step_frames * SUB), :] = (
                centered * lax.rsqrt(var + EPSILON)
            ).astype(jnp.bfloat16)

    norm(0)

    def project(j):
        @pl.loop(0, head)
        def _(h):
            r = jnp.dot(normed[...], w[j, h], preferred_element_type=jnp.float32)
            if j == 0:
                r = r * HS ** (-0.5)
            start = pl.multiple_of(h * columns, columns)
            qkv[j, :, pl.ds(start, columns)] = r.astype(jnp.bfloat16)

    parity_rows = pl.ds(
        pl.multiple_of(parity * half_seq * slice_rows, slice_rows), half_seq * slice_rows
    )
    for j in range(3):
        own[j].wait()
        drain(
            w.at[j, pl.ds(0, head - 1), pl.ds(0, (half_seq - 1) * slice_rows), :], s2_recv.at[j]
        )
        for i in range(1, head):
            piece = w.at[j, lax.rem(z + i, head), parity_rows, :]
            send(piece, piece, s3_send.at[j], s3_recv.at[j], sibling, z)
        if j == 1:
            for i in range(1, head):
                from_z = lax.rem(z + head - i, head)
                piece = w_o.at[
                    pl.ds(pl.multiple_of(from_z * shard + parity * half, half), half), :
                ]
                drain(piece, o1_recv.at[i - 1])
                send(piece, piece, o2_send, o2_recv, sibling, z)
        drain(w.at[j, pl.ds(0, head - 1), pl.ds(0, half_seq * slice_rows), :], s3_recv.at[j])
        project(j)

    own[3].wait()
    drain(w_o.at[pl.ds(0, (head - 1) * half), :], o2_recv)

    pair = 2 * HS
    left = lax.broadcasted_iota(jnp.int32, (rows, pair), 1) < HS
    left_b = left.astype(jnp.float32).astype(jnp.bfloat16)
    right_b = (1.0 - left.astype(jnp.float32)).astype(jnp.bfloat16)
    ones = jnp.ones((rows, pair), jnp.bfloat16)
    me = s * head + z

    def out_block(g):
        start = pl.multiple_of(z * quarter + s * own_patches + g * SUB, SUB)
        return out.at[:, pl.ds(start, SUB), :]

    def finish(g):
        @pl.loop(0, width // pair)
        def _(n):
            lanes = pl.ds(pl.multiple_of(n * pair, pair), pair)
            q, k, v = qkv[0, :, lanes], qkv[1, :, lanes], qkv[2, :, lanes]
            v_ones = jnp.concatenate([v, ones], axis=1)
            results = []
            for mask in (left_b, right_b):
                score = lax.dot_general(
                    q * mask, k, (((1,), (1,)), ((), ())), preferred_element_type=jnp.float32
                )
                score = score + bias[...]
                top = jnp.max(score, axis=1, keepdims=True)
                raised = jnp.exp(score - top).astype(jnp.bfloat16)
                r = jnp.dot(raised, v_ones, preferred_element_type=jnp.float32)
                results.append(r[:, :pair] / r[:, pair:])
            att[:, lanes] = jnp.where(left, results[0], results[1]).astype(jnp.bfloat16)

        @pl.loop(0, head)
        def _(h):
            lanes = pl.ds(pl.multiple_of(h * columns, columns), columns)
            r = jnp.dot(att[...], w_o[:, lanes], preferred_element_type=jnp.float32)
            mixed[g, pl.ds(h * frames, frames)] = r.reshape(frames, SUB, columns).astype(
                jnp.bfloat16
            )

        @pl.loop(1, total)
        def _(i):
            to = lax.rem(me + i, total)
            to_s, to_z = to // head, lax.rem(to, head)
            send(
                mixed.at[g, pl.ds(to_z * frames + to_s * own_frames, own_frames)],
                out_block(g), out_send.at[g], out_recv, to_s, to_z,
            )

        pltpu.make_async_copy(
            mixed.at[g, pl.ds(z * frames + s * own_frames, own_frames)], out_block(g), out_recv
        ).start()

    finish(0)

    @pl.loop(1, groups)
    def _(g):
        norm(g)
        for j in range(3):
            project(j)
        finish(g)

    drain(out, out_recv)
    blocks = head * frames
    for g in range(groups):
        drain(mixed.at[g, pl.ds(0, blocks - blocks // total)], out_send.at[g])
        drain(x.at[g, pl.ds(0, frames - own_frames)], tok_send.at[g])
    for j in range(3):
        drain(w.at[j, pl.ds(0, head - 1), pl.ds(0, slice_rows), :], s1_send.at[j])
        drain(
            w.at[j, pl.ds(0, head - 1), pl.ds(0, (half_seq - 1) * slice_rows), :], s2_send.at[j]
        )
        drain(w.at[j, pl.ds(0, head - 1), pl.ds(0, half_seq * slice_rows), :], s3_send.at[j])
    drain(w_o.at[pl.ds(0, (head - 1) * half), :], o1_send)
    drain(w_o.at[pl.ds(0, (head - 1) * half), :], o2_send)


def local(tokens, w_query, w_key, w_value, w_out):
    seq, head = lax.axis_size("seq"), lax.axis_size("head")
    own_frames, patches, width = tokens.shape
    frames = own_frames * seq
    groups = patches // (seq * head * SUB)
    rows = frames * SUB
    columns = w_query.shape[1]
    bf16 = jnp.bfloat16
    dma = pltpu.SemaphoreType.DMA
    return pl.pallas_call(
        functools.partial(kernel, seq, head),
        out_shape=jax.ShapeDtypeStruct((own_frames, patches, width // head), bf16),
        in_specs=[pl.BlockSpec(memory_space=pl.ANY)] * 5,
        out_specs=pl.BlockSpec(memory_space=pl.ANY),
        scratch_shapes=[
            pltpu.VMEM((groups, frames, SUB, width), bf16),
            pltpu.VMEM((rows, width), bf16),
            pltpu.VMEM((3, rows, width), bf16),
            pltpu.VMEM((3, head, width, columns), bf16),
            pltpu.VMEM((width, width), bf16),
            pltpu.VMEM((rows, width), bf16),
            pltpu.VMEM((groups, head * frames, SUB, width // head), bf16),
            pltpu.VMEM((rows, rows), jnp.float32),
            dma((groups,)), dma((groups,)), dma((4,)),
            dma((3,)), dma((3, head - 1)), dma((3,)), dma((3,)), dma((3,)), dma((3,)),
            dma, dma((head - 1,)), dma, dma, dma((groups,)), dma,
        ],
        compiler_params=pltpu.CompilerParams(
            has_side_effects=True, vmem_limit_bytes=60 * 1024 * 1024
        ),
    )(tokens, w_query, w_key, w_value, w_out)


def solution(mesh):
    return jax.shard_map(
        local,
        mesh=mesh,
        in_specs=(
            P("seq", None, None),
            P(None, "head"),
            P(None, "head"),
            P(None, "head"),
            P("head", None),
        ),
        out_specs=P("seq", None, "head"),
        check_vma=False,
    )
```

```python
import functools

import jax
import jax.numpy as jnp
from jax import lax
from jax.experimental import pallas as pl
from jax.experimental.pallas import tpu as pltpu
from jax.sharding import PartitionSpec as P

HS = 64
EPSILON = 1e-05
SUB = 8
MASKED = -1e30
MESH = pl.DeviceIdType.MESH


def drain(ref, sem):
    pltpu.make_async_copy(ref, ref, sem).wait()


def kernel(
    seq, head,
    tok, wq, wk, wv, wo, out,
    x, normed, qkv, w, w_o, att, mixed, bias,
    tok_send, tok_recv, load_sem, s1_send, s1_recv, s2_send, s2_recv, far_recv, s3_send, s3_recv,
    o1_send, o1_recv, o2_send, o2_recv, out_send, out_recv,
):
    s, z = lax.axis_index("seq"), lax.axis_index("head")
    groups, frames = x.shape[0], x.shape[1]
    own_frames = tok.shape[0]
    width = tok.shape[2]
    columns = wq.shape[1]
    rows = frames * SUB
    own_patches = groups * SUB
    quarter = seq * own_patches
    slice_rows = width // seq
    half_seq = seq // 2
    parity, place = lax.rem(s, 2), s // 2
    sibling = s + 1 - 2 * parity
    total = seq * head

    def send(src, dst, send_sem, recv_sem, to_s, to_z):
        pltpu.make_async_remote_copy(
            src_ref=src, dst_ref=dst, send_sem=send_sem, recv_sem=recv_sem,
            device_id=(to_s, to_z), device_id_type=MESH,
        ).start()

    def tok_block(to_s, g):
        start = pl.multiple_of(z * quarter + to_s * own_patches + g * SUB, SUB)
        return tok.at[:, pl.ds(start, SUB), :]

    slice_start = pl.multiple_of((parity * half_seq + place) * slice_rows, slice_rows)
    my_slice = pl.ds(slice_start, slice_rows)
    weights = (wq, wk, wv)
    def ways(d):
        return (
            (z - d, z - d >= 0, z + 1, z + 1 < head),
            (z + d, z + d < head, z - 1, z - 1 >= 0),
        )

    for j in range(3):
        for _, _, after, open_ in ways(1):

            @pl.when(open_)
            def _():
                send(
                    weights[j].at[my_slice, :], w.at[j, z, my_slice, :],
                    s1_send.at[j], s1_recv.at[j, z], s, after,
                )

    def exchange(g):
        for i in range(1, seq):
            to_s = lax.rem(s + i, seq)
            send(
                tok_block(to_s, g), x.at[g, pl.ds(s * own_frames, own_frames)],
                tok_send.at[g], tok_recv.at[g], to_s, z,
            )
        pltpu.make_async_copy(
            tok_block(s, g), x.at[g, pl.ds(s * own_frames, own_frames)], tok_recv.at[g]
        ).start()

    exchange(0)
    shard = width // head
    half = shard // 2
    def out_rows(from_z):
        return w_o.at[pl.ds(pl.multiple_of(from_z * shard + parity * half, half), half), :]

    for _, _, after, open_ in ways(1):

        @pl.when(open_)
        def _():
            send(
                wo.at[pl.ds(pl.multiple_of(parity * half, half), half), :],
                out_rows(z), o1_send, o1_recv.at[z], s, after,
            )

    own = [pltpu.make_async_copy(weights[j], w.at[j, z], load_sem.at[j]) for j in range(3)]
    own.append(
        pltpu.make_async_copy(
            wo, w_o.at[pl.ds(pl.multiple_of(z * shard, shard), shard), :], load_sem.at[3]
        )
    )
    for copy in own:
        copy.start()

    row = lax.broadcasted_iota(jnp.int32, (rows, rows), 0)
    col = lax.broadcasted_iota(jnp.int32, (rows, rows), 1)
    bias[...] = jnp.where((row & (SUB - 1)) == (col & (SUB - 1)), 0.0, MASKED)

    tall = max(n for n in range(1, half_seq + 1) if half_seq % n == 0 and n * n <= half_seq)
    wide = half_seq // tall
    up, across = place // wide, lax.rem(place, wide)

    def device_at(a, b):
        return (lax.rem(a, tall) * wide + lax.rem(b, wide)) * 2 + parity

    def rows_at(a, b, start, size):
        first = parity * half_seq + lax.rem(a, tall) * wide + lax.rem(b, wide)
        return pl.ds(pl.multiple_of(first * slice_rows + start, size), size)

    def spread(j):
        for d in range(1, head):
            for from_z, valid, after, open_ in ways(d):
                piece = w.at[j, jnp.clip(from_z, 0, head - 1), my_slice, :]
                arrived = s1_recv.at[j, jnp.clip(from_z, 0, head - 1)]

                @pl.when(valid)
                def _():
                    drain(piece, arrived)

                    @pl.when(open_)
                    def _():
                        send(piece, piece, s1_send.at[j], arrived, s, after)

                    for k in range(1, wide):
                        to_s = device_at(up, across + k)
                        send(piece, piece, s2_send.at[j], s2_recv.at[j, k - 1], to_s, z)
                    for k in range(1, tall):
                        to_s = device_at(up + k, across)
                        send(piece, piece, s2_send.at[j], s2_recv.at[j, wide + k - 2], to_s, z)

    half_rows = slice_rows // 2

    def relay(j):
        for k in range(1, wide):
            drain(w.at[j, pl.ds(0, head - 1), pl.ds(0, slice_rows), :], s2_recv.at[j, k - 1])
            for i in range(1, head):
                piece = w.at[
                    j, lax.rem(z + i, head), rows_at(up, across + wide - k, 0, half_rows), :
                ]
                for n in range(1, tall):
                    to_s = device_at(up + n, across)
                    send(piece, piece, s2_send.at[j], far_recv.at[j], to_s, z)
        for k in range(1, tall):
            drain(
                w.at[j, pl.ds(0, head - 1), pl.ds(0, slice_rows), :], s2_recv.at[j, wide + k - 2]
            )
            for i in range(1, head):
                piece = w.at[
                    j, lax.rem(z + i, head), rows_at(up + tall - k, across, half_rows, half_rows), :
                ]
                for n in range(1, wide):
                    to_s = device_at(up, across + n)
                    send(piece, piece, s2_send.at[j], far_recv.at[j], to_s, z)

    far = (tall - 1) * (wide - 1) * slice_rows
    parity_rows = pl.ds(
        pl.multiple_of(parity * half_seq * slice_rows, slice_rows), half_seq * slice_rows
    )

    def to_sibling(j):
        if far:
            drain(w.at[j, pl.ds(0, head - 1), pl.ds(0, far), :], far_recv.at[j])
        for i in range(1, head):
            piece = w.at[j, lax.rem(z + i, head), parity_rows, :]
            send(piece, piece, s3_send.at[j], s3_recv.at[j], sibling, z)

    def spread_out(d):
        for from_z, valid, after, open_ in ways(d):
            piece = out_rows(jnp.clip(from_z, 0, head - 1))
            arrived = o1_recv.at[jnp.clip(from_z, 0, head - 1)]

            @pl.when(valid)
            def _():
                drain(piece, arrived)

                @pl.when(open_)
                def _():
                    send(piece, piece, o1_send, arrived, s, after)

                send(piece, piece, o2_send, o2_recv, sibling, z)

    step_frames = 8

    def norm(g):
        drain(x.at[g], tok_recv.at[g])

        @pl.loop(0, frames // step_frames)
        def _(c):
            block = x[g, pl.ds(c * step_frames, step_frames)].astype(jnp.float32)
            values = block.reshape(step_frames * SUB, width)
            mean = jnp.mean(values, axis=-1, keepdims=True)
            centered = values - mean
            var = jnp.mean(centered * centered, axis=-1, keepdims=True)
            start = pl.multiple_of(c * step_frames * SUB, step_frames * SUB)
            normed[pl.ds(start, step_frames * SUB), :] = (
                centered * lax.rsqrt(var + EPSILON)
            ).astype(jnp.bfloat16)

    def project(j):
        @pl.loop(0, head)
        def _(h):
            r = jnp.dot(normed[...], w[j, h], preferred_element_type=jnp.float32)
            if j == 0:
                r = r * HS ** (-0.5)
            start = pl.multiple_of(h * columns, columns)
            qkv[j, :, pl.ds(start, columns)] = r.astype(jnp.bfloat16)

    def take(j):
        own[j].wait()
        drain(w.at[j, pl.ds(0, head - 1), pl.ds(0, half_seq * slice_rows), :], s3_recv.at[j])
        project(j)

    spread(0)
    spread(1)
    relay(0)
    spread(2)
    norm(0)
    spread_out(1)
    relay(1)
    to_sibling(0)
    for d in range(2, head - 1):
        spread_out(d)
    relay(2)
    for g in range(1, groups):
        exchange(g)
    to_sibling(1)
    take(0)
    if head > 2:
        spread_out(head - 1)
    take(1)
    to_sibling(2)
    take(2)
    own[3].wait()
    drain(w_o.at[pl.ds(0, (head - 1) * half), :], o2_recv)

    pair = 2 * HS
    left = lax.broadcasted_iota(jnp.int32, (rows, pair), 1) < HS
    left_b = left.astype(jnp.float32).astype(jnp.bfloat16)
    right_b = (1.0 - left.astype(jnp.float32)).astype(jnp.bfloat16)
    ones = jnp.ones((rows, pair), jnp.bfloat16)
    me = s * head + z

    def out_block(g):
        start = pl.multiple_of(z * quarter + s * own_patches + g * SUB, SUB)
        return out.at[:, pl.ds(start, SUB), :]

    def finish(g):
        @pl.loop(0, width // pair)
        def _(n):
            lanes = pl.ds(pl.multiple_of(n * pair, pair), pair)
            q, k, v = qkv[0, :, lanes], qkv[1, :, lanes], qkv[2, :, lanes]
            v_ones = jnp.concatenate([v, ones], axis=1)
            results = []
            for mask in (left_b, right_b):
                score = lax.dot_general(
                    q * mask, k, (((1,), (1,)), ((), ())), preferred_element_type=jnp.float32
                )
                score = score + bias[...]
                top = jnp.max(score, axis=1, keepdims=True)
                raised = jnp.exp(score - top).astype(jnp.bfloat16)
                r = jnp.dot(raised, v_ones, preferred_element_type=jnp.float32)
                results.append(r[:, :pair] / r[:, pair:])
            att[:, lanes] = jnp.where(left, results[0], results[1]).astype(jnp.bfloat16)

        @pl.loop(0, head)
        def _(h):
            lanes = pl.ds(pl.multiple_of(h * columns, columns), columns)
            r = jnp.dot(att[...], w_o[:, lanes], preferred_element_type=jnp.float32)
            mixed[g, pl.ds(h * frames, frames)] = r.reshape(frames, SUB, columns).astype(
                jnp.bfloat16
            )

        @pl.loop(1, total)
        def _(i):
            to = lax.rem(me + i, total)
            to_s, to_z = to // head, lax.rem(to, head)
            send(
                mixed.at[g, pl.ds(to_z * frames + to_s * own_frames, own_frames)],
                out_block(g), out_send.at[g], out_recv, to_s, to_z,
            )

        pltpu.make_async_copy(
            mixed.at[g, pl.ds(z * frames + s * own_frames, own_frames)], out_block(g), out_recv
        ).start()

    finish(0)

    @pl.loop(1, groups)
    def _(g):
        norm(g)
        for j in range(3):
            project(j)
        finish(g)

    drain(out, out_recv)
    blocks = head * frames
    for g in range(groups):
        drain(mixed.at[g, pl.ds(0, blocks - blocks // total)], out_send.at[g])
        drain(x.at[g, pl.ds(0, frames - own_frames)], tok_send.at[g])
    for j in range(3):
        for d in range(head):
            for from_z, valid, _, open_ in ways(d):

                @pl.when(valid & open_)
                def _():
                    drain(w.at[j, 0, pl.ds(0, slice_rows), :], s1_send.at[j])

        drain(
            w.at[j, pl.ds(0, head - 1), pl.ds(0, (half_seq - 1) * slice_rows), :], s2_send.at[j]
        )
        drain(w.at[j, pl.ds(0, head - 1), pl.ds(0, half_seq * slice_rows), :], s3_send.at[j])
    for d in range(head):
        for from_z, valid, _, open_ in ways(d):

            @pl.when(valid & open_)
            def _():
                drain(w_o.at[pl.ds(0, half), :], o1_send)

    drain(w_o.at[pl.ds(0, (head - 1) * half), :], o2_send)


def local(tokens, w_query, w_key, w_value, w_out):
    seq, head = lax.axis_size("seq"), lax.axis_size("head")
    own_frames, patches, width = tokens.shape
    frames = own_frames * seq
    groups = patches // (seq * head * SUB)
    rows = frames * SUB
    columns = w_query.shape[1]
    bf16 = jnp.bfloat16
    dma = pltpu.SemaphoreType.DMA
    return pl.pallas_call(
        functools.partial(kernel, seq, head),
        out_shape=jax.ShapeDtypeStruct((own_frames, patches, width // head), bf16),
        in_specs=[pl.BlockSpec(memory_space=pl.ANY)] * 5,
        out_specs=pl.BlockSpec(memory_space=pl.ANY),
        scratch_shapes=[
            pltpu.VMEM((groups, frames, SUB, width), bf16),
            pltpu.VMEM((rows, width), bf16),
            pltpu.VMEM((3, rows, width), bf16),
            pltpu.VMEM((3, head, width, columns), bf16),
            pltpu.VMEM((width, width), bf16),
            pltpu.VMEM((rows, width), bf16),
            pltpu.VMEM((groups, head * frames, SUB, width // head), bf16),
            pltpu.VMEM((rows, rows), jnp.float32),
            dma((groups,)), dma((groups,)), dma((4,)),
            dma((3,)), dma((3, head)), dma((3,)), dma((3, seq // 2)), dma((3,)), dma((3,)), dma((3,)),
            dma, dma((head,)), dma, dma, dma((groups,)), dma,
        ],
        compiler_params=pltpu.CompilerParams(
            has_side_effects=True, vmem_limit_bytes=60 * 1024 * 1024
        ),
    )(tokens, w_query, w_key, w_value, w_out)


def solution(mesh):
    return jax.shard_map(
        local,
        mesh=mesh,
        in_specs=(
            P("seq", None, None),
            P(None, "head"),
            P(None, "head"),
            P(None, "head"),
            P("head", None),
        ),
        out_specs=P("seq", None, "head"),
        check_vma=False,
    )
```

```python
import functools

import jax
import jax.numpy as jnp
from jax import lax
from jax.experimental import pallas as pl
from jax.experimental.pallas import tpu as pltpu
from jax.sharding import PartitionSpec as P

HS = 64
EPSILON = 1e-05
SUB = 8
MASKED = -1e30
MESH = pl.DeviceIdType.MESH


def drain(ref, sem):
    pltpu.make_async_copy(ref, ref, sem).wait()


def kernel(
    seq, head,
    tok, wq, wk, wv, wo, out,
    x, normed, qkv, w, w_o, att, mixed, bias,
    tok_send, tok_recv, load_sem, s1_send, s1_recv, s2_send, s2_recv, far_recv, s3_send, s3_recv,
    o1_send, o1_recv, o2_send, o2_recv, out_send, out_recv,
):
    s, z = lax.axis_index("seq"), lax.axis_index("head")
    groups, frames = x.shape[0], x.shape[1]
    own_frames = tok.shape[0]
    width = tok.shape[2]
    columns = wq.shape[1]
    rows = frames * SUB
    own_patches = groups * SUB
    quarter = seq * own_patches
    slice_rows = width // seq
    half_seq = seq // 2
    parity, place = lax.rem(s, 2), s // 2
    sibling = s + 1 - 2 * parity
    total = seq * head

    def send(src, dst, send_sem, recv_sem, to_s, to_z):
        pltpu.make_async_remote_copy(
            src_ref=src, dst_ref=dst, send_sem=send_sem, recv_sem=recv_sem,
            device_id=(to_s, to_z), device_id_type=MESH,
        ).start()

    def tok_block(to_s, g):
        start = pl.multiple_of(z * quarter + to_s * own_patches + g * SUB, SUB)
        return tok.at[:, pl.ds(start, SUB), :]

    slice_start = pl.multiple_of((parity * half_seq + place) * slice_rows, slice_rows)
    my_slice = pl.ds(slice_start, slice_rows)
    weights = (wq, wk, wv)
    def ways(d):
        return (
            (z - d, z - d >= 0, z + 1, z + 1 < head),
            (z + d, z + d < head, z - 1, z - 1 >= 0),
        )

    for j in range(3):
        for _, _, after, open_ in ways(1):

            @pl.when(open_)
            def _():
                send(
                    weights[j].at[my_slice, :], w.at[j, z, my_slice, :],
                    s1_send.at[j], s1_recv.at[j, z], s, after,
                )

    def exchange(g):
        for i in range(1, seq):
            to_s = lax.rem(s + i, seq)
            send(
                tok_block(to_s, g), x.at[g, pl.ds(s * own_frames, own_frames)],
                tok_send.at[g], tok_recv.at[g], to_s, z,
            )
        pltpu.make_async_copy(
            tok_block(s, g), x.at[g, pl.ds(s * own_frames, own_frames)], tok_recv.at[g]
        ).start()

    exchange(0)
    shard = width // head
    half = shard // 2
    def out_rows(from_z):
        return w_o.at[pl.ds(pl.multiple_of(from_z * shard + parity * half, half), half), :]

    for _, _, after, open_ in ways(1):

        @pl.when(open_)
        def _():
            send(
                wo.at[pl.ds(pl.multiple_of(parity * half, half), half), :],
                out_rows(z), o1_send, o1_recv.at[z], s, after,
            )

    own = [pltpu.make_async_copy(weights[j], w.at[j, z], load_sem.at[j]) for j in range(3)]
    own.append(
        pltpu.make_async_copy(
            wo, w_o.at[pl.ds(pl.multiple_of(z * shard, shard), shard), :], load_sem.at[3]
        )
    )
    for copy in own:
        copy.start()

    row = lax.broadcasted_iota(jnp.int32, (rows, rows), 0)
    col = lax.broadcasted_iota(jnp.int32, (rows, rows), 1)
    bias[...] = jnp.where((row & (SUB - 1)) == (col & (SUB - 1)), 0.0, MASKED)

    tall = max(n for n in range(1, half_seq + 1) if half_seq % n == 0 and n * n <= half_seq)
    wide = half_seq // tall
    up, across = place // wide, lax.rem(place, wide)

    def device_at(a, b):
        return (lax.rem(a, tall) * wide + lax.rem(b, wide)) * 2 + parity

    def rows_at(a, b, start, size):
        first = parity * half_seq + lax.rem(a, tall) * wide + lax.rem(b, wide)
        return pl.ds(pl.multiple_of(first * slice_rows + start, size), size)

    def spread(j):
        for d in range(1, head):
            for from_z, valid, after, open_ in ways(d):
                piece = w.at[j, jnp.clip(from_z, 0, head - 1), my_slice, :]
                arrived = s1_recv.at[j, jnp.clip(from_z, 0, head - 1)]

                @pl.when(valid)
                def _():
                    drain(piece, arrived)

                    @pl.when(open_)
                    def _():
                        send(piece, piece, s1_send.at[j], arrived, s, after)

                    for k in range(1, wide):
                        to_s = device_at(up, across + k)
                        send(piece, piece, s2_send.at[j], s2_recv.at[j, k - 1], to_s, z)
                    for k in range(1, tall):
                        to_s = device_at(up + k, across)
                        send(piece, piece, s2_send.at[j], s2_recv.at[j, wide + k - 2], to_s, z)

    half_rows = slice_rows // 2

    def relay(j):
        for k in range(1, wide):
            drain(w.at[j, pl.ds(0, head - 1), pl.ds(0, slice_rows), :], s2_recv.at[j, k - 1])
            for i in range(1, head):
                piece = w.at[
                    j, lax.rem(z + i, head), rows_at(up, across + wide - k, 0, half_rows), :
                ]
                for n in range(1, tall):
                    to_s = device_at(up + n, across)
                    send(piece, piece, s2_send.at[j], far_recv.at[j], to_s, z)
        for k in range(1, tall):
            drain(
                w.at[j, pl.ds(0, head - 1), pl.ds(0, slice_rows), :], s2_recv.at[j, wide + k - 2]
            )
            for i in range(1, head):
                piece = w.at[
                    j, lax.rem(z + i, head), rows_at(up + tall - k, across, half_rows, half_rows), :
                ]
                for n in range(1, wide):
                    to_s = device_at(up, across + n)
                    send(piece, piece, s2_send.at[j], far_recv.at[j], to_s, z)

    far = (tall - 1) * (wide - 1) * slice_rows
    parity_rows = pl.ds(
        pl.multiple_of(parity * half_seq * slice_rows, slice_rows), half_seq * slice_rows
    )

    def to_sibling(j):
        if far:
            drain(w.at[j, pl.ds(0, head - 1), pl.ds(0, far), :], far_recv.at[j])
        for i in range(1, head):
            piece = w.at[j, lax.rem(z + i, head), parity_rows, :]
            send(piece, piece, s3_send.at[j], s3_recv.at[j], sibling, z)

    def spread_out(d):
        for from_z, valid, after, open_ in ways(d):
            piece = out_rows(jnp.clip(from_z, 0, head - 1))
            arrived = o1_recv.at[jnp.clip(from_z, 0, head - 1)]

            @pl.when(valid)
            def _():
                drain(piece, arrived)

                @pl.when(open_)
                def _():
                    send(piece, piece, o1_send, arrived, s, after)

                send(piece, piece, o2_send, o2_recv, sibling, z)

    step_frames = 8

    def norm(g):
        drain(x.at[g], tok_recv.at[g])

        @pl.loop(0, frames // step_frames)
        def _(c):
            block = x[g, pl.ds(c * step_frames, step_frames)].astype(jnp.float32)
            values = block.reshape(step_frames * SUB, width)
            mean = jnp.mean(values, axis=-1, keepdims=True)
            centered = values - mean
            var = jnp.mean(centered * centered, axis=-1, keepdims=True)
            start = pl.multiple_of(c * step_frames * SUB, step_frames * SUB)
            normed[pl.ds(start, step_frames * SUB), :] = (
                centered * lax.rsqrt(var + EPSILON)
            ).astype(jnp.bfloat16)

    def project(j):
        @pl.loop(0, head, unroll=True)
        def _(h):
            r = jnp.dot(normed[...], w[j, h], preferred_element_type=jnp.float32)
            if j == 0:
                r = r * HS ** (-0.5)
            start = pl.multiple_of(h * columns, columns)
            qkv[j, :, pl.ds(start, columns)] = r.astype(jnp.bfloat16)

    def take(j):
        own[j].wait()
        drain(w.at[j, pl.ds(0, head - 1), pl.ds(0, half_seq * slice_rows), :], s3_recv.at[j])
        project(j)

    spread(0)
    spread(1)
    relay(0)
    spread(2)
    norm(0)
    spread_out(1)
    relay(1)
    to_sibling(0)
    for d in range(2, head - 1):
        spread_out(d)
    relay(2)
    for g in range(1, groups):
        exchange(g)
    to_sibling(1)
    take(0)
    take(1)
    to_sibling(2)
    take(2)
    if head > 2:
        spread_out(head - 1)
    pair = 2 * HS
    left = lax.broadcasted_iota(jnp.int32, (rows, pair), 1) < HS
    left_b = left.astype(jnp.float32).astype(jnp.bfloat16)
    right_b = (1.0 - left.astype(jnp.float32)).astype(jnp.bfloat16)
    ones = jnp.ones((rows, pair), jnp.bfloat16)
    me = s * head + z

    def out_block(g):
        start = pl.multiple_of(z * quarter + s * own_patches + g * SUB, SUB)
        return out.at[:, pl.ds(start, SUB), :]

    def finish(g, first=False):
        @pl.loop(0, width // pair, unroll=4)
        def _(n):
            lanes = pl.ds(pl.multiple_of(n * pair, pair), pair)
            q, k, v = qkv[0, :, lanes], qkv[1, :, lanes], qkv[2, :, lanes]
            v_ones = jnp.concatenate([v, ones], axis=1)
            results = []
            for mask in (left_b, right_b):
                score = lax.dot_general(
                    q * mask, k, (((1,), (1,)), ((), ())), preferred_element_type=jnp.float32
                )
                score = score + bias[...]
                top = jnp.max(score, axis=1, keepdims=True)
                raised = jnp.exp(score - top).astype(jnp.bfloat16)
                r = jnp.dot(raised, v_ones, preferred_element_type=jnp.float32)
                results.append(r[:, :pair] / r[:, pair:])
            att[:, lanes] = jnp.where(left, results[0], results[1]).astype(jnp.bfloat16)

        if first:
            own[3].wait()
            drain(w_o.at[pl.ds(0, (head - 1) * half), :], o2_recv)

        @pl.loop(0, head, unroll=True)
        def _(h):
            lanes = pl.ds(pl.multiple_of(h * columns, columns), columns)
            r = jnp.dot(att[...], w_o[:, lanes], preferred_element_type=jnp.float32)
            mixed[g, pl.ds(h * frames, frames)] = r.reshape(frames, SUB, columns).astype(
                jnp.bfloat16
            )

        @pl.loop(1, total)
        def _(i):
            to = lax.rem(me + i, total)
            to_s, to_z = to // head, lax.rem(to, head)
            send(
                mixed.at[g, pl.ds(to_z * frames + to_s * own_frames, own_frames)],
                out_block(g), out_send.at[g], out_recv, to_s, to_z,
            )

        pltpu.make_async_copy(
            mixed.at[g, pl.ds(z * frames + s * own_frames, own_frames)], out_block(g), out_recv
        ).start()

    finish(0, True)

    @pl.loop(1, groups)
    def _(g):
        norm(g)
        for j in range(3):
            project(j)
        finish(g)

    drain(out, out_recv)
    blocks = head * frames
    for g in range(groups):
        drain(mixed.at[g, pl.ds(0, blocks - blocks // total)], out_send.at[g])
        drain(x.at[g, pl.ds(0, frames - own_frames)], tok_send.at[g])
    for j in range(3):
        for d in range(head):
            for from_z, valid, _, open_ in ways(d):

                @pl.when(valid & open_)
                def _():
                    drain(w.at[j, 0, pl.ds(0, slice_rows), :], s1_send.at[j])

        drain(
            w.at[j, pl.ds(0, head - 1), pl.ds(0, (half_seq - 1) * slice_rows), :], s2_send.at[j]
        )
        drain(w.at[j, pl.ds(0, head - 1), pl.ds(0, half_seq * slice_rows), :], s3_send.at[j])
    for d in range(head):
        for from_z, valid, _, open_ in ways(d):

            @pl.when(valid & open_)
            def _():
                drain(w_o.at[pl.ds(0, half), :], o1_send)

    drain(w_o.at[pl.ds(0, (head - 1) * half), :], o2_send)


def local(tokens, w_query, w_key, w_value, w_out):
    seq, head = lax.axis_size("seq"), lax.axis_size("head")
    own_frames, patches, width = tokens.shape
    frames = own_frames * seq
    groups = patches // (seq * head * SUB)
    rows = frames * SUB
    columns = w_query.shape[1]
    bf16 = jnp.bfloat16
    dma = pltpu.SemaphoreType.DMA
    return pl.pallas_call(
        functools.partial(kernel, seq, head),
        out_shape=jax.ShapeDtypeStruct((own_frames, patches, width // head), bf16),
        in_specs=[pl.BlockSpec(memory_space=pl.ANY)] * 5,
        out_specs=pl.BlockSpec(memory_space=pl.ANY),
        scratch_shapes=[
            pltpu.VMEM((groups, frames, SUB, width), bf16),
            pltpu.VMEM((rows, width), bf16),
            pltpu.VMEM((3, rows, width), bf16),
            pltpu.VMEM((3, head, width, columns), bf16),
            pltpu.VMEM((width, width), bf16),
            pltpu.VMEM((rows, width), bf16),
            pltpu.VMEM((groups, head * frames, SUB, width // head), bf16),
            pltpu.VMEM((rows, rows), jnp.float32),
            dma((groups,)), dma((groups,)), dma((4,)),
            dma((3,)), dma((3, head)), dma((3,)), dma((3, seq // 2)), dma((3,)), dma((3,)), dma((3,)),
            dma, dma((head,)), dma, dma, dma((groups,)), dma,
        ],
        compiler_params=pltpu.CompilerParams(
            has_side_effects=True, vmem_limit_bytes=60 * 1024 * 1024
        ),
    )(tokens, w_query, w_key, w_value, w_out)


def solution(mesh):
    return jax.shard_map(
        local,
        mesh=mesh,
        in_specs=(
            P("seq", None, None),
            P(None, "head"),
            P(None, "head"),
            P(None, "head"),
            P("head", None),
        ),
        out_specs=P("seq", None, "head"),
        check_vma=False,
    )
```
